1024 devices in a mesh: cell: 64 (over y, x_hi, core), state: 16 (over z, x_lo).
Axes of the slice: x: 8 (x_hi: 4, x_lo: 2; x = x_hi * 2 + x_lo), y: 8, z: 8, core: 2. Of those that a mesh axis runs over, the one named last changes fastest.
Arguments:
- start_block: float32 [1024, 32768], P('state', 'cell'), may hold values from -6 to 6
- connectivity: int32 [128, 343], P('cell'), may hold values from 0 to 575, as said below
- cell_matrices: bfloat16 [128, 343, 343], P('cell'), may hold values from -4 to 4
- bounds: float32 [3], replicated, may hold values from -1 to 32, as said below
Outputs:
- filtered: float32 [1024, 32768], P('state', 'cell')
- projected: float32 [1024, 1024], P('cell', 'state')
The draws below stay inside these ranges and needn't reach their ends.
Inputs may be any that keep to these rules, and one draw needn't show every extreme that they name: `connectivity`: each row names 343 different local nodes; numbers below 512 are nodes owned by the index of cell that holds the cell, the others the first 64 nodes of the next index of cell, cyclically. `bounds`: lowest < cut < upper, and every eigenvalue of H lies above lowest.
All inputs are finite; a program needn't handle non-finite values.
Results may differ from the reference program's by a relative error of at most 0.0016.
Values may be sent and summed in bfloat16 or wider, within the bound.
No kernel may reach another device: no remote copies, remote signals or barrier semaphores. Data moves between devices by JAX's collectives and lax.ppermute only.
A program may use at most 32 MiB of HBM per device.

```python
import jax
import jax.numpy as jnp
from jax import lax

NSTATES = 1024
NPC = 343
DEGREE = 8
CELLS_DEV = 2
NODE_DEV = 512
HALO = 64
NCELLS = 128
NODES = 32768
N_CELL = 64


def draw_connectivity(key, part):
    extent = NODE_DEV + HALO
    scores = jax.random.randint(key, (NCELLS, extent), 0, 2 ** 20) * extent + jnp.arange(extent, dtype=jnp.int32)[None, :]
    order = jnp.argsort(scores, axis=1, stable=True)
    return order[:, :NPC].astype(jnp.int32)


def draw_cell_matrices(key, part):
    key_off = jax.random.fold_in(key, 11)
    key_diag = jax.random.fold_in(key, 12)
    noise = jax.random.normal(key_off, (NCELLS, NPC, NPC), jnp.float32)
    diag = jax.random.uniform(key_diag, (NCELLS, NPC), jnp.float32, 1.5, 3.5)
    sym = (noise + jnp.swapaxes(noise, 1, 2)) * (0.5 / jnp.sqrt(2.0 * NPC))
    eye = jnp.eye(NPC, dtype=jnp.float32)
    matrix = sym * (1.0 - eye)[None] + diag[:, :, None] * eye[None]
    return matrix.astype(jnp.bfloat16)


def draw_bounds(key, part):
    parts = jax.random.uniform(key, (3,), jnp.float32, 0.0, 1.0)
    lowest = -1.0 + 0.5 * parts[0]
    cut = 4.0 + 2.0 * parts[1]
    upper = 28.0 + 4.0 * parts[2]
    return jnp.stack([lowest, cut, upper]).astype(jnp.float32)


def shard_levels(stream_key, shape, split, low, largest):
    factor_of = 1.0
    for position, shards_of in split:
        steps = jax.random.uniform(jax.random.fold_in(jax.random.fold_in(stream_key, 6), position), (shards_of,), jnp.float32, low / len(split), largest / len(split))
        factor_of = factor_of * jnp.repeat(jnp.exp(steps), shape[position] // shards_of).reshape((-1,) + (1,) * (len(shape) - 1 - position))
    return factor_of


def centred(key, dims, deviation, limit, split=(), held_as=jnp.bfloat16):
    gain = shard_levels(key, dims, split, -0.22, 0.18) if split else 1.0
    array = jax.random.normal(key, dims, jnp.float32) * deviation * gain
    return jnp.minimum(jnp.maximum(array, -limit), limit).astype(held_as)


def setup_inputs(seed: int = 0) -> dict:
    key_list = jax.random.split(jax.random.key(seed), 5)
    return {
        "start_block": centred(key_list[0], (NSTATES, NODES), 1.0, 6.0, ((0, 16), (1, 64)), jnp.float32),
        "connectivity": draw_connectivity(jax.random.fold_in(key_list[4], 71), 0),
        "cell_matrices": draw_cell_matrices(jax.random.fold_in(key_list[4], 71), 0),
        "bounds": draw_bounds(jax.random.fold_in(key_list[4], 71), 0),
    }


def apply_operator(field, connectivity, cell_matrices):
    states = field.shape[0]
    blocks = field.astype(jnp.bfloat16).reshape(states, N_CELL, NODE_DEV).transpose(1, 0, 2)
    ghost = jnp.roll(blocks[:, :, :HALO], -1, axis=0)
    extended = jnp.concatenate([blocks, ghost], axis=2)
    links = connectivity.reshape(N_CELL, CELLS_DEV, NPC)
    locals_ = cell_matrices.reshape(N_CELL, CELLS_DEV, NPC, NPC)

    def one_index(item):
        ext, link, matrix = item
        picked = ext[:, link].astype(jnp.float32)
        product = jnp.einsum("scj,ckj->sck", picked, matrix.astype(jnp.float32), precision=lax.Precision.HIGHEST)
        return jnp.zeros(ext.shape, jnp.float32).at[:, link].add(product)

    sums = lax.map(one_index, (extended, links, locals_))
    owned = sums[:, :, :NODE_DEV]
    incoming = jnp.roll(sums[:, :, NODE_DEV:], 1, axis=0)
    owned = owned.at[:, :, :HALO].add(incoming)
    return owned.transpose(1, 0, 2).reshape(states, N_CELL * NODE_DEV)


def reference(start_block, connectivity, cell_matrices, bounds):
    lowest, cut, upper = bounds[0], bounds[1], bounds[2]
    half = (upper - cut) / 2.0
    centre = (upper + cut) / 2.0
    sigma = half / (lowest - centre)
    tau = 2.0 / sigma
    previous = start_block
    current = (apply_operator(start_block, connectivity, cell_matrices) - centre * start_block) * (sigma / half)
    for degree in range(2, DEGREE + 1):
        sigma_new = 1.0 / (tau - sigma)
        upcoming = (apply_operator(current, connectivity, cell_matrices) - centre * current) * (2.0 * sigma_new / half) - (sigma * sigma_new) * previous
        previous = current
        current = upcoming
        sigma = sigma_new
    low = current.astype(jnp.bfloat16)
    image = apply_operator(current, connectivity, cell_matrices).astype(jnp.bfloat16)
    projected = jnp.dot(low, image.T, preferred_element_type=jnp.float32)
    return current, projected
```

```python
import functools

import jax
import jax.numpy as jnp
from jax import lax
from jax.experimental import pallas as pl
from jax.experimental.pallas import tpu as pltpu
from jax.sharding import PartitionSpec as P

DEGREE = 8


def passed_along(value, axis, steps):
    count = lax.axis_size(axis)
    pairs = [(source, (source + steps) % count) for source in range(count)]
    return lax.ppermute(value, axis, pairs)


def swapped(value, axis, first):
    count = lax.axis_size(axis)
    pairs = []
    for low in range(first, first + count, 2):
        left, right = low % count, (low + 1) % count
        pairs += [(left, right), (right, left)]
    return lax.ppermute(value, axis, pairs)


def scattered(connectivity, cell_matrices, extent):
    nodes = lax.broadcasted_iota(jnp.int32, (*connectivity.shape, extent), 2)
    chosen = (connectivity[:, :, None] == nodes).astype(jnp.bfloat16)
    half = jnp.einsum(
        "cba,cbk->cak", cell_matrices, chosen, preferred_element_type=jnp.float32
    ).astype(jnp.bfloat16)
    whole = jnp.einsum("cai,cak->cik", chosen, half, preferred_element_type=jnp.float32)
    cells = connectivity.shape[0]
    return whole.astype(jnp.bfloat16).reshape(cells * extent, extent)


def completed(flag, own, ghost, chip, link):
    even = flag[0] == 0
    first = ghost.shape[1]
    left = jnp.where(even, link, chip)
    right = jnp.where(even, chip, link)
    return own[:, :first] + left, ghost + right


def multiplied(extended, weights, cells):
    extent = weights.shape[0] // cells
    total = None
    for cell in range(cells):
        part = jnp.dot(
            extended,
            weights[cell * extent : (cell + 1) * extent, :],
            preferred_element_type=jnp.float32,
        )
        total = part if total is None else total + part
    return total


def degree_body(cells, flag, coef, own, ghost, chip, link, previous, weights, current, upcoming, spill, to_chip, to_link, extended):
    shared, owned = ghost.shape[1], own.shape[1]
    left, right = completed(flag, own[...], ghost[...], chip[...], link[...])
    current[...] = own[...]
    current[:, :shared] = left
    values = current[...]
    extended[:, :owned] = values.astype(jnp.bfloat16)
    extended[:, owned:] = right.astype(jnp.bfloat16)
    product = multiplied(extended[...], weights, cells)
    fresh = coef[0] * product[:, :owned] + coef[1] * values + coef[2] * previous[...]
    beyond = coef[0] * product[:, owned:]
    upcoming[...] = fresh
    spill[...] = beyond
    even = flag[0] == 0
    first = fresh[:, :shared]
    to_chip[...] = jnp.where(even, beyond, first)
    to_link[...] = jnp.where(even, first, beyond)


def image_body(cells, flag, own, ghost, chip, link, weights, current, low, product_out, spill, extended):
    shared, owned = ghost.shape[1], own.shape[1]
    left, right = completed(flag, own[...], ghost[...], chip[...], link[...])
    current[...] = own[...]
    current[:, :shared] = left
    values = current[...].astype(jnp.bfloat16)
    low[...] = values
    extended[:, :owned] = values
    extended[:, owned:] = right.astype(jnp.bfloat16)
    product = multiplied(extended[...], weights, cells)
    product_out[...] = product[:, :owned]
    spill[...] = product[:, owned:]


def project_body(lows, product, incoming, out):
    states, shared = incoming.shape
    value = product[...]
    first = value[:, :shared] + incoming[...]
    image = jnp.concatenate([first, value[:, shared:]], axis=1).astype(jnp.bfloat16)
    partial = lax.dot_general(
        lows[...], image, (((1,), (1,)), ((), ())), preferred_element_type=jnp.float32
    )
    pieces = partial.reshape(partial.shape[0] // 16, 2, 8, states)
    out[...] = jnp.concatenate([pieces[:, 0], pieces[:, 1]], axis=2)


def in_smem(count):
    return [pl.BlockSpec(memory_space=pltpu.SMEM)] * count


def in_vmem(count):
    return [pl.BlockSpec(memory_space=pltpu.VMEM)] * count


def per_device(start_block, connectivity, cell_matrices, bounds):
    f32 = jnp.float32
    states, owned = start_block.shape
    shared = owned // 8
    extent = owned + shared
    cells = connectivity.shape[0]
    flag = (lax.axis_index("cell") % 2).astype(jnp.int32).reshape(1)
    weights = scattered(connectivity, cell_matrices, extent)

    whole = jax.ShapeDtypeStruct((states, owned), f32)
    group = jax.ShapeDtypeStruct((states, shared), f32)
    scratch = [pltpu.VMEM((states, extent), jnp.bfloat16)]
    step = pl.pallas_call(
        functools.partial(degree_body, cells),
        in_specs=in_smem(2) + in_vmem(6),
        out_specs=tuple(in_vmem(5)),
        out_shape=(whole, whole, group, group, group),
        scratch_shapes=scratch,
        name="degree",
    )
    last = pl.pallas_call(
        functools.partial(image_body, cells),
        in_specs=in_smem(1) + in_vmem(5),
        out_specs=tuple(in_vmem(4)),
        out_shape=(whole, jax.ShapeDtypeStruct((states, owned), jnp.bfloat16), whole, group),
        scratch_shapes=scratch,
        name="image",
    )

    lowest, cut, upper = (bounds[0], bounds[1], bounds[2])
    half = (upper - cut) / 2.0
    centre = (upper + cut) / 2.0
    sigma = half / (lowest - centre)
    tau = 2.0 / sigma
    coefs = [jnp.stack([sigma / half, -centre * (sigma / half), jnp.zeros((), f32)])]
    for degree in range(2, DEGREE + 1):
        sigma_new = 1.0 / (tau - sigma)
        scale = 2.0 * sigma_new / half
        coefs.append(jnp.stack([scale, -centre * scale, -(sigma * sigma_new)]))
        sigma = sigma_new

    ghost = passed_along(start_block[:, :shared].astype(jnp.bfloat16), "cell", -1).astype(f32)
    own, previous = start_block, start_block
    chip = link = jnp.zeros((states, shared), f32)
    for coef in coefs:
        previous, own, ghost, to_chip, to_link = step(
            flag, coef, own, ghost, chip, link, previous, weights
        )
        chip = swapped(to_chip, "cell", 0)
        link = swapped(to_link, "cell", 1)
    filtered, low, product, spill = last(flag, own, ghost, chip, link, weights)
    incoming = passed_along(spill, "cell", 1)
    peers = lax.axis_size("state")
    lows = lax.all_to_all(
        jnp.broadcast_to(low[None], (peers, states, owned)), "state", 0, 0, tiled=True
    ).reshape(peers * states, owned)

    count = lax.axis_size("cell")
    rows = peers * states // count
    pieces = pl.pallas_call(
        project_body,
        in_specs=in_vmem(3),
        out_specs=in_vmem(1)[0],
        out_shape=jax.ShapeDtypeStruct((peers * states // 16, 8, 2 * states), f32),
        name="project",
    )(lows, product, incoming)
    arrived = lax.all_to_all(pieces, "cell", 0, 0, tiled=True)
    total = jnp.sum(arrived.reshape(count, rows // 16, 8, 2, states), axis=0)
    projected = jnp.swapaxes(total, 1, 2).reshape(rows, states)
    return (filtered, projected)


def solution(mesh):
    in_specs = (P("state", "cell"), P("cell", None), P("cell", None, None), P())
    out_specs = (P("state", "cell"), P("cell", "state"))
    return jax.shard_map(
        per_device, mesh=mesh, in_specs=in_specs, out_specs=out_specs, check_vma=False
    )
```

```python
import functools

import jax
import jax.numpy as jnp
from jax import lax
from jax.experimental import pallas as pl
from jax.experimental.pallas import tpu as pltpu
from jax.sharding import PartitionSpec as P

DEGREE = 8


def passed_along(value, axis, steps):
    count = lax.axis_size(axis)
    pairs = [(source, (source + steps) % count) for source in range(count)]
    return lax.ppermute(value, axis, pairs)


def swapped(value, axis, first):
    count = lax.axis_size(axis)
    pairs = []
    for low in range(first, first + count, 2):
        left, right = low % count, (low + 1) % count
        pairs += [(left, right), (right, left)]
    return lax.ppermute(value, axis, pairs)


def scattered(connectivity, cell_matrices, extent):
    nodes = lax.broadcasted_iota(jnp.int32, (*connectivity.shape, extent), 2)
    chosen = (connectivity[:, :, None] == nodes).astype(jnp.bfloat16)
    half = jnp.einsum(
        "cba,cbk->cak", cell_matrices, chosen, preferred_element_type=jnp.float32
    ).astype(jnp.bfloat16)
    whole = jnp.einsum("cai,cak->cik", chosen, half, preferred_element_type=jnp.float32)
    return whole.astype(jnp.bfloat16)


def completed(flag, own, ghost, chip, link):
    even = flag[0] == 0
    first = ghost.shape[1]
    left = jnp.where(even, link, chip)
    right = jnp.where(even, chip, link)
    return own[:, :first] + left, ghost + right


def multiplied(extended, weights, cells):
    total = None
    for cell in range(cells):
        part = jnp.dot(
            extended,
            weights[cell],
            preferred_element_type=jnp.float32,
        )
        total = part if total is None else total + part
    return total


def advanced(cells, flag, coef, values, right, previous, weights, upcoming, spill, to_chip, to_link, extended):
    shared, owned = right.shape[1], values.shape[1]
    extended[:, :owned] = values.astype(jnp.bfloat16)
    extended[:, owned:] = right.astype(jnp.bfloat16)
    product = multiplied(extended[...], weights, cells)
    fresh = coef[0] * product[:, :owned] + coef[1] * values
    if previous is not None:
        fresh = fresh + coef[2] * previous
    beyond = coef[0] * product[:, owned:]
    upcoming[...] = fresh
    spill[...] = beyond
    even = flag[0] == 0
    first = fresh[:, :shared]
    to_chip[...] = jnp.where(even, beyond, first)
    to_link[...] = jnp.where(even, first, beyond)


def first_body(cells, flag, coef, start, ghost, weights, upcoming, spill, to_chip, to_link, extended):
    advanced(cells, flag, coef, start[...], ghost[...], None, weights, upcoming, spill, to_chip, to_link, extended)


def degree_body(cells, flag, coef, own, ghost, chip, link, previous, weights, current, upcoming, spill, to_chip, to_link, extended):
    shared = ghost.shape[1]
    left, right = completed(flag, own[...], ghost[...], chip[...], link[...])
    current[...] = own[...]
    current[:, :shared] = left
    advanced(cells, flag, coef, current[...], right, previous[...], weights, upcoming, spill, to_chip, to_link, extended)


def image_body(cells, flag, own, ghost, chip, link, weights, current, low, product_out, spill, extended):
    shared, owned = ghost.shape[1], own.shape[1]
    left, right = completed(flag, own[...], ghost[...], chip[...], link[...])
    current[...] = own[...]
    current[:, :shared] = left
    values = current[...].astype(jnp.bfloat16)
    low[...] = jnp.broadcast_to(values[None], low.shape)
    extended[:, :owned] = values
    extended[:, owned:] = right.astype(jnp.bfloat16)
    product = multiplied(extended[...], weights, cells)
    product_out[...] = product[:, :owned]
    spill[...] = product[:, owned:]


def project_body(lows, product, incoming, out):
    states, shared = incoming.shape
    value = product[...]
    first = value[:, :shared] + incoming[...]
    image = jnp.concatenate([first, value[:, shared:]], axis=1).astype(jnp.bfloat16)
    partial = lax.dot_general(
        lows[...], image, (((1,), (1,)), ((), ())), preferred_element_type=jnp.float32
    )
    pieces = partial.reshape(partial.shape[0] // 16, 2, 8, states)
    out[...] = jnp.concatenate([pieces[:, 0], pieces[:, 1]], axis=2)


def kernel(body, cells, scalars, out_shape, scratch):
    def run(*operands):
        small, large = operands[:scalars], operands[scalars:]
        large = [pltpu.with_memory_space_constraint(value, pltpu.VMEM) for value in large]
        in_specs = [pl.BlockSpec(memory_space=pltpu.SMEM)] * scalars
        in_specs += [pl.BlockSpec(memory_space=pltpu.VMEM)] * len(large)
        single = not isinstance(out_shape, tuple)
        outs = pl.BlockSpec(memory_space=pltpu.VMEM)
        return pl.pallas_call(
            functools.partial(body, cells) if cells else body,
            in_specs=in_specs,
            out_specs=outs if single else (outs,) * len(out_shape),
            out_shape=out_shape,
            scratch_shapes=scratch,
            compiler_params=pltpu.CompilerParams(vmem_limit_bytes=16 * 2**20),
        )(*small, *large)

    return run


def exchanged(to_link, to_chip):
    link = swapped(to_link, "cell", 1)
    chip = swapped(to_chip, "cell", 0)
    return link, chip


def per_device(start_block, connectivity, cell_matrices, bounds):
    f32 = jnp.float32
    states, owned = start_block.shape
    shared = owned // 8
    extent = owned + shared
    cells = connectivity.shape[0]
    flag = (lax.axis_index("cell") % 2).astype(jnp.int32).reshape(1)
    weights = scattered(connectivity, cell_matrices, extent)

    peers = lax.axis_size("state")
    whole = pltpu.VMEM((states, owned), f32)
    group = pltpu.VMEM((states, shared), f32)
    bf16 = jnp.bfloat16
    scratch = [pltpu.VMEM((states, extent), bf16)]
    first = kernel(first_body, cells, 2, (whole, group, group, group), scratch)
    step = kernel(degree_body, cells, 2, (whole, whole, group, group, group), scratch)
    out = jax.ShapeDtypeStruct((states, owned), f32)
    lows = pltpu.VMEM((peers, states, owned), bf16)
    last = kernel(image_body, cells, 1, (out, lows, whole, group), scratch)

    lowest, cut, upper = (bounds[0], bounds[1], bounds[2])
    half = (upper - cut) / 2.0
    centre = (upper + cut) / 2.0
    sigma = half / (lowest - centre)
    tau = 2.0 / sigma
    coefs = [jnp.stack([sigma / half, -centre * (sigma / half), jnp.zeros((), f32)])]
    for _ in range(2, DEGREE + 1):
        sigma_new = 1.0 / (tau - sigma)
        scale = 2.0 * sigma_new / half
        coefs.append(jnp.stack([scale, -centre * scale, -(sigma * sigma_new)]))
        sigma = sigma_new

    ghost = passed_along(start_block[:, :shared].astype(bf16), "cell", -1)
    own, ghost, to_chip, to_link = first(flag, coefs[0], start_block, ghost, weights)
    previous = start_block
    for coef in coefs[1:]:
        link, chip = exchanged(to_link, to_chip)
        previous, own, ghost, to_chip, to_link = step(
            flag, coef, own, ghost, chip, link, previous, weights
        )
    link, chip = exchanged(to_link, to_chip)
    filtered, low, product, spill = last(flag, own, ghost, chip, link, weights)
    incoming = passed_along(spill, "cell", 1)
    lows = lax.all_to_all(low, "state", 0, 0, tiled=True)
    lows = lows.reshape(peers * states, owned)

    count = lax.axis_size("cell")
    rows = peers * states // count
    shape = pltpu.VMEM((peers * states // 16, 8, 2 * states), f32)
    pieces = kernel(project_body, 0, 0, shape, [])(lows, product, incoming)
    arrived = lax.all_to_all(pieces, "cell", 0, 0, tiled=True)
    total = jnp.sum(arrived.reshape(count, rows // 16, 8, 2, states), axis=0)
    projected = jnp.swapaxes(total, 1, 2).reshape(rows, states)
    return (filtered, projected)


def solution(mesh):
    in_specs = (P("state", "cell"), P("cell", None), P("cell", None, None), P())
    out_specs = (P("state", "cell"), P("cell", "state"))
    return jax.shard_map(
        per_device, mesh=mesh, in_specs=in_specs, out_specs=out_specs, check_vma=False
    )
```

```python
import functools

import jax
import jax.numpy as jnp
from jax import lax
from jax.experimental import pallas as pl
from jax.experimental.pallas import tpu as pltpu
from jax.sharding import PartitionSpec as P

DEGREE = 8


def passed_along(value, axis, steps):
    count = lax.axis_size(axis)
    pairs = [(source, (source + steps) % count) for source in range(count)]
    return lax.ppermute(value, axis, pairs)


def swapped(value, axis, first):
    count = lax.axis_size(axis)
    pairs = []
    for low in range(first, first + count, 2):
        left, right = low % count, (low + 1) % count
        pairs += [(left, right), (right, left)]
    return lax.ppermute(value, axis, pairs)


def scattered(connectivity, cell_matrices, extent):
    nodes = lax.broadcasted_iota(jnp.int32, (*connectivity.shape, extent), 2)
    chosen = (connectivity[:, :, None] == nodes).astype(jnp.bfloat16)
    half = jnp.einsum(
        "cba,cbk->cak", cell_matrices, chosen, preferred_element_type=jnp.float32
    ).astype(jnp.bfloat16)
    whole = jnp.einsum("cai,cak->cik", chosen, half, preferred_element_type=jnp.float32)
    return whole.astype(jnp.bfloat16)


def completed(flag, own, ghost, chip, link):
    even = flag[0] == 0
    first = ghost.shape[1]
    left = jnp.where(even, link, chip)
    right = jnp.where(even, chip, link)
    return own[:, :first] + left, ghost + right


def multiplied(extended, weights, cells):
    total = None
    for cell in range(cells):
        part = jnp.dot(
            extended,
            weights[cell],
            preferred_element_type=jnp.float32,
        )
        total = part if total is None else total + part
    return total


def advanced(cells, flag, coef, values, right, previous, weights, upcoming, spill, to_chip, to_link, extended):
    shared, owned = right.shape[1], values.shape[1]
    extended[:, :owned] = values.astype(jnp.bfloat16)
    extended[:, owned:] = right.astype(jnp.bfloat16)
    product = multiplied(extended[...], weights, cells)
    fresh = coef[0] * product[:, :owned] + coef[1] * values
    if previous is not None:
        fresh = fresh + coef[2] * previous
    beyond = coef[0] * product[:, owned:]
    upcoming[...] = fresh
    spill[...] = beyond
    even = flag[0] == 0
    first = fresh[:, :shared]
    to_chip[...] = jnp.where(even, beyond, first)
    to_link[...] = jnp.where(even, first, beyond)


def first_body(cells, flag, coef, start, ghost, weights, upcoming, spill, to_chip, to_link, extended):
    advanced(cells, flag, coef, start[...], ghost[...], None, weights, upcoming, spill, to_chip, to_link, extended)


def degree_body(cells, flag, coef, own, ghost, chip, link, previous, weights, current, upcoming, spill, to_chip, to_link, extended):
    shared = ghost.shape[1]
    left, right = completed(flag, own[...], ghost[...], chip[...], link[...])
    current[...] = own[...]
    current[:, :shared] = left
    advanced(cells, flag, coef, current[...], right, previous[...], weights, upcoming, spill, to_chip, to_link, extended)


def image_body(cells, flag, own, ghost, chip, link, weights, current, low, product_out, spill, extended):
    shared, owned = ghost.shape[1], own.shape[1]
    left, right = completed(flag, own[...], ghost[...], chip[...], link[...])
    current[...] = own[...]
    current[:, :shared] = left
    values = current[...].astype(jnp.bfloat16)
    low[...] = jnp.broadcast_to(values[None], low.shape)
    extended[:, :owned] = values
    extended[:, owned:] = right.astype(jnp.bfloat16)
    product = multiplied(extended[...], weights, cells)
    product_out[...] = product[:, :owned]
    spill[...] = product[:, owned:]


def finish_body(product, incoming, image):
    shared = incoming.shape[1]
    image[...] = product[...].astype(jnp.bfloat16)
    image[:, :shared] = (product[:, :shared] + incoming[...]).astype(jnp.bfloat16)


def project_body(flag, lows, image, neighbour, keep, handed):
    states = image.shape[0]
    images = jnp.concatenate([image[...], neighbour[...]], axis=0)
    partial = lax.dot_general(
        lows[...], images, (((1,), (1,)), ((), ())), preferred_element_type=jnp.float32
    )
    rows = partial.reshape(partial.shape[0] // 32, 2, 2, 8, 2 * states)
    even = flag[0] == 0
    mine = jnp.where(even, rows[:, 0], rows[:, 1])
    other = jnp.where(even, rows[:, 1], rows[:, 0])
    for place, value in ((keep, mine), (handed, other)):
        place[0] = jnp.concatenate([value[:, 0, :, :states], value[:, 1, :, :states]], axis=2)
        place[1] = jnp.concatenate([value[:, 0, :, states:], value[:, 1, :, states:]], axis=2)


def add_body(keep, received, own, other):
    own[...] = keep[0] + received[0]
    other[...] = keep[1] + received[1]


def place_body(half, own, received, out):
    low = half[0] == 0
    groups = out.shape[0]
    mine = own[...].reshape(groups, 2, *own.shape[1:])
    theirs = received[...].reshape(groups, 2, *own.shape[1:])
    out[:, 0] = jnp.where(low, mine, theirs)
    out[:, 1] = jnp.where(low, theirs, mine)


def kernel(body, cells, scalars, out_shape, scratch):
    def run(*operands):
        small, large = operands[:scalars], operands[scalars:]
        large = [pltpu.with_memory_space_constraint(value, pltpu.VMEM) for value in large]
        in_specs = [pl.BlockSpec(memory_space=pltpu.SMEM)] * scalars
        in_specs += [pl.BlockSpec(memory_space=pltpu.VMEM)] * len(large)
        single = not isinstance(out_shape, tuple)
        outs = pl.BlockSpec(memory_space=pltpu.VMEM)
        return pl.pallas_call(
            functools.partial(body, cells) if cells else body,
            in_specs=in_specs,
            out_specs=outs if single else (outs,) * len(out_shape),
            out_shape=out_shape,
            scratch_shapes=scratch,
            compiler_params=pltpu.CompilerParams(vmem_limit_bytes=16 * 2**20),
        )(*small, *large)

    return run


def alternate(count):
    return [list(range(first, count, 2)) for first in range(2)]


def exchanged(to_link, to_chip):
    link = swapped(to_link, "cell", 1)
    chip = swapped(to_chip, "cell", 0)
    return link, chip


def per_device(start_block, connectivity, cell_matrices, bounds):
    f32 = jnp.float32
    states, owned = start_block.shape
    shared = owned // 8
    extent = owned + shared
    cells = connectivity.shape[0]
    flag = (lax.axis_index("cell") % 2).astype(jnp.int32).reshape(1)
    weights = scattered(connectivity, cell_matrices, extent)

    peers = lax.axis_size("state")
    whole = pltpu.VMEM((states, owned), f32)
    group = pltpu.VMEM((states, shared), f32)
    bf16 = jnp.bfloat16
    scratch = [pltpu.VMEM((states, extent), bf16)]
    first = kernel(first_body, cells, 2, (whole, group, group, group), scratch)
    step = kernel(degree_body, cells, 2, (whole, whole, group, group, group), scratch)
    out = jax.ShapeDtypeStruct((states, owned), f32)
    line = peers // 2
    lows = pltpu.VMEM((line, states, owned), bf16)
    last = kernel(image_body, cells, 1, (out, lows, whole, group), scratch)

    lowest, cut, upper = (bounds[0], bounds[1], bounds[2])
    half = (upper - cut) / 2.0
    centre = (upper + cut) / 2.0
    sigma = half / (lowest - centre)
    tau = 2.0 / sigma
    coefs = [jnp.stack([sigma / half, -centre * (sigma / half), jnp.zeros((), f32)])]
    for _ in range(2, DEGREE + 1):
        sigma_new = 1.0 / (tau - sigma)
        scale = 2.0 * sigma_new / half
        coefs.append(jnp.stack([scale, -centre * scale, -(sigma * sigma_new)]))
        sigma = sigma_new

    ghost = passed_along(start_block[:, :shared].astype(bf16), "cell", -1)
    own, ghost, to_chip, to_link = first(flag, coefs[0], start_block, ghost, weights)
    previous = start_block
    for number, coef in enumerate(coefs[1:]):
        link, chip = exchanged(to_link, to_chip)
        previous, own, ghost, to_chip, to_link = step(
            flag, coef, own, ghost, chip, link, previous, weights
        )
    link, chip = exchanged(to_link, to_chip)
    filtered, low, product, spill = last(flag, own, ghost, chip, link, weights)
    incoming = passed_along(spill, "cell", 1)
    lows = lax.all_to_all(
        low, "state", 0, 0, axis_index_groups=alternate(peers), tiled=True
    )
    lows = lows.reshape(line * states, owned)
    shape = pltpu.VMEM((states, owned), bf16)
    image = kernel(finish_body, 0, 0, shape, [])(product, incoming)
    neighbour = swapped(image, "state", 0)

    count = lax.axis_size("cell")
    half = (lax.axis_index("state") % 2).astype(jnp.int32).reshape(1)
    number = line * states // 32
    both = pltpu.VMEM((2, number, 8, 2 * states), f32)
    keep, handed = kernel(project_body, 0, 1, (both, both), [])(
        flag, lows, image, neighbour
    )
    part = pltpu.VMEM((number, 8, 2 * states), f32)
    own, other = kernel(add_body, 0, 0, (part, part), [])(keep, swapped(handed, "cell", 0))
    received = swapped(other, "state", 0)
    shape = pltpu.VMEM((number // 2, 2, 2, 8, 2 * states), f32)
    pieces = kernel(place_body, 0, 1, shape, [])(half, own, received)
    pieces = pieces.reshape(2 * number, 8, 2 * states)
    arrived = lax.all_to_all(
        pieces, "cell", 0, 0, axis_index_groups=alternate(count), tiled=True
    )
    rows = peers * states // count
    total = jnp.sum(arrived.reshape(count // 2, rows // 16, 8, 2, states), axis=0)
    projected = jnp.swapaxes(total, 1, 2).reshape(rows, states)
    return (filtered, projected)


def solution(mesh):
    in_specs = (P("state", "cell"), P("cell", None), P("cell", None, None), P())
    out_specs = (P("state", "cell"), P("cell", "state"))
    return jax.shard_map(
        per_device, mesh=mesh, in_specs=in_specs, out_specs=out_specs, check_vma=False
    )
```

```python
import jax
import jax.numpy as jnp
from jax import lax
from jax.experimental import pallas as pl
from jax.experimental.pallas import tpu as pltpu
from jax.sharding import PartitionSpec as P

DEGREE = 8


def passed_along(value, axis, steps):
    count = lax.axis_size(axis)
    pairs = [(source, (source + steps) % count) for source in range(count)]
    return lax.ppermute(value, axis, pairs)


def swapped(value, axis, first):
    count = lax.axis_size(axis)
    pairs = []
    for low in range(first, first + count, 2):
        left, right = low % count, (low + 1) % count
        pairs += [(left, right), (right, left)]
    return lax.ppermute(value, axis, pairs)


def scattered(connectivity, cell_matrices, owned, shared):
    index = lax.broadcasted_iota(jnp.int32, (*connectivity.shape, owned + shared), 2)
    rest = jnp.where(index < 2 * shared, index + owned - shared, index - shared)
    nodes = jnp.where(index < shared, index, rest)
    chosen = (connectivity[:, :, None] == nodes).astype(jnp.bfloat16)
    half = jnp.einsum(
        "cba,cbk->cak", cell_matrices, chosen, preferred_element_type=jnp.float32
    ).astype(jnp.bfloat16)
    whole = jnp.einsum("cai,cak->cik", chosen, half, preferred_element_type=jnp.float32)
    return whole.astype(jnp.bfloat16)


def turned(value):
    middle = value.shape[1] // 2
    return jnp.concatenate([value[:, middle:], value[:, :middle]], axis=1)


def in_own(value):
    return lax.broadcasted_iota(jnp.int32, value.shape, 1) < value.shape[1] // 2


def completed(flag, fresh, link, chip):
    even = flag[0] == 0
    link, chip = turned(link), turned(chip)
    left = jnp.where(even, link, chip)
    right = jnp.where(even, chip, link)
    return fresh + jnp.where(in_own(fresh), left, right)


def fill(extended, edge, inner):
    width = edge.shape[1]
    extended[:, :width] = edge.astype(jnp.bfloat16)
    extended[:, width:] = inner.astype(jnp.bfloat16)


def multiplied(extended, weights, begin, end):
    total = None
    for cell in range(weights.shape[0]):
        part = jnp.dot(
            extended[...], weights[cell, :, begin:end], preferred_element_type=jnp.float32
        )
        total = part if total is None else total + part
    return total


def first_body(coef, start, ghost, weights, edge, inner, upcoming, extended):
    shared = ghost.shape[1]
    values = jnp.concatenate([start[:, :shared], ghost[...].astype(jnp.float32)], axis=1)
    edge[...] = values
    inner[...] = start[:, shared:]
    fill(extended, values, inner[...])
    product = multiplied(extended, weights, 0, 2 * shared)
    upcoming[...] = coef[0] * product + jnp.where(in_own(values), coef[1] * values, 0.0)


def edge_body(flag, coef, fresh, link, chip, inner, before, weights, edge, upcoming, extended):
    values = completed(flag, fresh[...], link[...], chip[...])
    edge[...] = values
    fill(extended, values, inner[...])
    product = multiplied(extended, weights, 0, values.shape[1])
    kept = coef[1] * values + coef[2] * before[...]
    upcoming[...] = coef[0] * product + jnp.where(in_own(values), kept, 0.0)


def inner_body(coef, edge, inner, weights, *rest):
    before, upcoming, extended = rest if len(rest) == 3 else (None, *rest)
    fill(extended, edge[...], inner[...])
    product = multiplied(extended, weights, edge.shape[1], weights.shape[2])
    fresh = coef[0] * product + coef[1] * inner[...]
    if before is not None:
        fresh = fresh + coef[2] * before[...]
    upcoming[...] = fresh


def last_edge_body(flag, fresh, link, chip, inner, weights, edge, low, product, extended):
    values = completed(flag, fresh[...], link[...], chip[...])
    edge[...] = values
    fill(extended, values, inner[...])
    shared = values.shape[1] // 2
    rounded = jnp.concatenate([inner[...], values[:, :shared]], axis=1).astype(jnp.bfloat16)
    low[...] = jnp.broadcast_to(rounded[None], low.shape)
    product[...] = multiplied(extended, weights, 0, values.shape[1])


def last_inner_body(edge, inner, weights, filtered, product, extended):
    shared = edge.shape[1] // 2
    fill(extended, edge[...], inner[...])
    product[...] = multiplied(extended, weights, edge.shape[1], weights.shape[2])
    filtered[...] = jnp.concatenate([edge[:, :shared], inner[...]], axis=1)


def finish_body(edge, inner, incoming, image):
    shared = edge.shape[1] // 2
    first = edge[:, :shared] + incoming[:, shared:]
    image[...] = jnp.concatenate([inner[...], first], axis=1).astype(jnp.bfloat16)


def project_body(flag, lows, image, neighbour, keep, handed):
    states = image.shape[0]
    images = jnp.concatenate([image[...], neighbour[...]], axis=0)
    partial = lax.dot_general(
        lows[...], images, (((1,), (1,)), ((), ())), preferred_element_type=jnp.float32
    )
    rows = partial.reshape(partial.shape[0] // 32, 2, 2, 8, 2 * states)
    even = flag[0] == 0
    mine = jnp.where(even, rows[:, 0], rows[:, 1])
    other = jnp.where(even, rows[:, 1], rows[:, 0])
    for place, value in ((keep, mine), (handed, other)):
        place[0] = jnp.concatenate([value[:, 0, :, :states], value[:, 1, :, :states]], axis=2)
        place[1] = jnp.concatenate([value[:, 0, :, states:], value[:, 1, :, states:]], axis=2)


def add_body(keep, received, own, other):
    own[...] = keep[0] + received[0]
    other[...] = keep[1] + received[1]


def place_body(half, own, received, out):
    low = half[0] == 0
    groups = out.shape[0]
    mine = own[...].reshape(groups, 2, *own.shape[1:])
    theirs = received[...].reshape(groups, 2, *own.shape[1:])
    out[:, 0] = jnp.where(low, mine, theirs)
    out[:, 1] = jnp.where(low, theirs, mine)


def kernel(body, scalars, out_shape, scratch):
    def run(*operands):
        small, large = operands[:scalars], operands[scalars:]
        large = [pltpu.with_memory_space_constraint(value, pltpu.VMEM) for value in large]
        in_specs = [pl.BlockSpec(memory_space=pltpu.SMEM)] * scalars
        in_specs += [pl.BlockSpec(memory_space=pltpu.VMEM)] * len(large)
        single = not isinstance(out_shape, tuple)
        outs = pl.BlockSpec(memory_space=pltpu.VMEM)
        return pl.pallas_call(
            body,
            in_specs=in_specs,
            out_specs=outs if single else (outs,) * len(out_shape),
            out_shape=out_shape,
            scratch_shapes=scratch,
            compiler_params=pltpu.CompilerParams(vmem_limit_bytes=16 * 2**20),
        )(*small, *large)

    return run


def alternate(count):
    return [list(range(first, count, 2)) for first in range(2)]


def exchanged(value):
    link = swapped(value, "cell", 1)
    chip = swapped(value, "cell", 0)
    return link, chip


def per_device(start_block, connectivity, cell_matrices, bounds):
    f32 = jnp.float32
    states, owned = start_block.shape
    shared = owned // 8
    extent = owned + shared
    flag = (lax.axis_index("cell") % 2).astype(jnp.int32).reshape(1)
    weights = scattered(connectivity, cell_matrices, owned, shared)

    peers = lax.axis_size("state")
    line = peers // 2
    bf16 = jnp.bfloat16
    rim = pltpu.VMEM((states, 2 * shared), f32)
    core = pltpu.VMEM((states, owned - shared), f32)
    scratch = [pltpu.VMEM((states, extent), bf16)]
    first = kernel(first_body, 1, (rim, core, rim), scratch)
    edge_step = kernel(edge_body, 2, (rim, rim), scratch)
    inner_step = kernel(inner_body, 1, core, scratch)
    lows = pltpu.VMEM((line, states, owned), bf16)
    last_edge = kernel(last_edge_body, 1, (rim, lows, rim), scratch)
    out = jax.ShapeDtypeStruct((states, owned), f32)
    last_inner = kernel(last_inner_body, 0, (out, core), scratch)

    lowest, cut, upper = (bounds[0], bounds[1], bounds[2])
    half = (upper - cut) / 2.0
    centre = (upper + cut) / 2.0
    sigma = half / (lowest - centre)
    tau = 2.0 / sigma
    coefs = [jnp.stack([sigma / half, -centre * (sigma / half), jnp.zeros((), f32)])]
    for _ in range(2, DEGREE + 1):
        sigma_new = 1.0 / (tau - sigma)
        scale = 2.0 * sigma_new / half
        coefs.append(jnp.stack([scale, -centre * scale, -(sigma * sigma_new)]))
        sigma = sigma_new

    ghost = passed_along(start_block[:, :shared].astype(bf16), "cell", -1)
    edge, inner, fresh = first(coefs[0], start_block, ghost, weights)
    before = ()
    for number, coef in enumerate(coefs):
        link, chip = exchanged(fresh)
        upcoming = inner_step(coef, edge, inner, weights, *before)
        before, inner = (inner,), upcoming
        if number + 1 < len(coefs):
            edge, fresh = edge_step(
                flag, coefs[number + 1], fresh, link, chip, inner, edge, weights
            )
    edge, low, edge_product = last_edge(flag, fresh, link, chip, inner, weights)
    incoming = passed_along(edge_product, "cell", 1)
    lows = lax.all_to_all(low, "state", 0, 0, axis_index_groups=alternate(peers), tiled=True)
    filtered, inner_product = last_inner(edge, inner, weights)
    lows = lows.reshape(line * states, owned)
    shape = pltpu.VMEM((states, owned), bf16)
    image = kernel(finish_body, 0, shape, [])(
        edge_product, inner_product, incoming
    )
    neighbour = swapped(image, "state", 0)

    count = lax.axis_size("cell")
    half = (lax.axis_index("state") % 2).astype(jnp.int32).reshape(1)
    number = line * states // 32
    both = pltpu.VMEM((2, number, 8, 2 * states), f32)
    keep, handed = kernel(project_body, 1, (both, both), [])(flag, lows, image, neighbour)
    part = pltpu.VMEM((number, 8, 2 * states), f32)
    own, other = kernel(add_body, 0, (part, part), [])(keep, swapped(handed, "cell", 0))
    received = swapped(other, "state", 0)
    shape = pltpu.VMEM((number // 2, 2, 2, 8, 2 * states), f32)
    pieces = kernel(place_body, 1, shape, [])(half, own, received)
    pieces = pieces.reshape(2 * number, 8, 2 * states)
    arrived = lax.all_to_all(
        pieces, "cell", 0, 0, axis_index_groups=alternate(count), tiled=True
    )
    rows = peers * states // count
    total = jnp.sum(arrived.reshape(count // 2, rows // 16, 8, 2, states), axis=0)
    projected = jnp.swapaxes(total, 1, 2).reshape(rows, states)
    return (filtered, projected)


def solution(mesh):
    in_specs = (P("state", "cell"), P("cell", None), P("cell", None, None), P())
    out_specs = (P("state", "cell"), P("cell", "state"))
    return jax.shard_map(
        per_device, mesh=mesh, in_specs=in_specs, out_specs=out_specs, check_vma=False
    )
```

```python
import jax
import jax.numpy as jnp
from jax import lax
from jax.experimental import pallas as pl
from jax.experimental.pallas import tpu as pltpu
from jax.sharding import PartitionSpec as P

DEGREE = 8


def passed_along(value, axis, steps):
    count = lax.axis_size(axis)
    pairs = [(source, (source + steps) % count) for source in range(count)]
    return lax.ppermute(value, axis, pairs)


def swapped(value, axis, first):
    count = lax.axis_size(axis)
    pairs = []
    for low in range(first, first + count, 2):
        left, right = low % count, (low + 1) % count
        pairs += [(left, right), (right, left)]
    return lax.ppermute(value, axis, pairs)


def scattered(connectivity, cell_matrices, owned, shared):
    index = lax.broadcasted_iota(jnp.int32, (*connectivity.shape, owned + shared), 2)
    rest = jnp.where(index < 2 * shared, index + owned - shared, index - shared)
    nodes = jnp.where(index < shared, index, rest)
    chosen = (connectivity[:, :, None] == nodes).astype(jnp.bfloat16)
    half = jnp.einsum(
        "cba,cbk->cak", cell_matrices, chosen, preferred_element_type=jnp.float32
    ).astype(jnp.bfloat16)
    whole = jnp.einsum("cai,cak->cik", chosen, half, preferred_element_type=jnp.float32)
    return whole.astype(jnp.bfloat16)


def turned(value):
    middle = value.shape[1] // 2
    return jnp.concatenate([value[:, middle:], value[:, :middle]], axis=1)


def in_own(value):
    return lax.broadcasted_iota(jnp.int32, value.shape, 1) < value.shape[1] // 2


def completed(flag, fresh, link, chip):
    even = flag[0] == 0
    link, chip = turned(link), turned(chip)
    left = jnp.where(even, link, chip)
    right = jnp.where(even, chip, link)
    return fresh + jnp.where(in_own(fresh), left, right)


def fill(extended, edge, inner):
    width = edge.shape[1]
    extended[:, :width] = edge.astype(jnp.bfloat16)
    extended[:, width:] = inner.astype(jnp.bfloat16)


def multiplied(values, weights, begin, end, row=0):
    total = None
    stop = row + values.shape[1]
    for cell in range(weights.shape[0]):
        part = jnp.dot(
            values, weights[cell, row:stop, begin:end], preferred_element_type=jnp.float32
        )
        total = part if total is None else total + part
    return total


def first_body(coef, start, ghost, weights, edge, inner, upcoming, extended):
    shared = ghost.shape[1]
    values = jnp.concatenate([start[:, :shared], ghost[...].astype(jnp.float32)], axis=1)
    edge[...] = values
    inner[...] = start[:, shared:]
    fill(extended, values, inner[...])
    product = multiplied(extended[...], weights, 0, 2 * shared)
    upcoming[...] = coef[0] * product + jnp.where(in_own(values), coef[1] * values, 0.0)


def edge_body(flag, coef, fresh, link, chip, ahead, before, weights, edge, upcoming):
    values = completed(flag, fresh[...], link[...], chip[...])
    edge[...] = values
    width = values.shape[1]
    product = ahead[...] + multiplied(values.astype(jnp.bfloat16), weights, 0, width)
    kept = coef[1] * values + coef[2] * before[...]
    upcoming[...] = coef[0] * product + jnp.where(in_own(values), kept, 0.0)


def inner_body(coef, edge, inner, weights, *rest):
    before, upcoming, ahead, extended = rest if len(rest) == 4 else (None, *rest)
    width = edge.shape[1]
    fill(extended, edge[...], inner[...])
    product = multiplied(extended[...], weights, width, weights.shape[2])
    fresh = coef[0] * product + coef[1] * inner[...]
    if before is not None:
        fresh = fresh + coef[2] * before[...]
    upcoming[...] = fresh
    ahead[...] = multiplied(fresh.astype(jnp.bfloat16), weights, 0, width, width)


def last_edge_body(flag, fresh, link, chip, inner, ahead, weights, edge, low, product):
    values = completed(flag, fresh[...], link[...], chip[...])
    edge[...] = values
    width = values.shape[1]
    rounded = jnp.concatenate([inner[...], values[:, : width // 2]], axis=1).astype(jnp.bfloat16)
    low[...] = jnp.broadcast_to(rounded[None], low.shape)
    product[...] = ahead[...] + multiplied(values.astype(jnp.bfloat16), weights, 0, width)


def last_inner_body(edge, inner, weights, filtered, product, extended):
    shared = edge.shape[1] // 2
    fill(extended, edge[...], inner[...])
    product[...] = multiplied(extended[...], weights, edge.shape[1], weights.shape[2])
    filtered[...] = jnp.concatenate([edge[:, :shared], inner[...]], axis=1)


def finish_body(edge, inner, incoming, image):
    shared = edge.shape[1] // 2
    first = edge[:, :shared] + incoming[:, shared:]
    image[...] = jnp.concatenate([inner[...], first], axis=1).astype(jnp.bfloat16)


def project_body(flag, lows, image, neighbour, keep, handed):
    states = image.shape[0]
    images = jnp.concatenate([image[...], neighbour[...]], axis=0)
    partial = lax.dot_general(
        lows[...], images, (((1,), (1,)), ((), ())), preferred_element_type=jnp.float32
    )
    rows = partial.reshape(partial.shape[0] // 32, 2, 2, 8, 2 * states)
    even = flag[0] == 0
    mine = jnp.where(even, rows[:, 0], rows[:, 1])
    other = jnp.where(even, rows[:, 1], rows[:, 0])
    for place, value in ((keep, mine), (handed, other)):
        place[0] = jnp.concatenate([value[:, 0, :, :states], value[:, 1, :, :states]], axis=2)
        place[1] = jnp.concatenate([value[:, 0, :, states:], value[:, 1, :, states:]], axis=2)


def add_body(keep, received, own, other):
    own[...] = keep[0] + received[0]
    other[...] = keep[1] + received[1]


def place_body(half, own, received, out):
    low = half[0] == 0
    groups = out.shape[0]
    mine = own[...].reshape(groups, 2, *own.shape[1:])
    theirs = received[...].reshape(groups, 2, *own.shape[1:])
    out[:, 0] = jnp.where(low, mine, theirs)
    out[:, 1] = jnp.where(low, theirs, mine)


def kernel(body, scalars, out_shape, scratch):
    def run(*operands):
        small, large = operands[:scalars], operands[scalars:]
        large = [pltpu.with_memory_space_constraint(value, pltpu.VMEM) for value in large]
        in_specs = [pl.BlockSpec(memory_space=pltpu.SMEM)] * scalars
        in_specs += [pl.BlockSpec(memory_space=pltpu.VMEM)] * len(large)
        single = not isinstance(out_shape, tuple)
        outs = pl.BlockSpec(memory_space=pltpu.VMEM)
        return pl.pallas_call(
            body,
            in_specs=in_specs,
            out_specs=outs if single else (outs,) * len(out_shape),
            out_shape=out_shape,
            scratch_shapes=scratch,
            compiler_params=pltpu.CompilerParams(vmem_limit_bytes=16 * 2**20),
        )(*small, *large)

    return run


def alternate(count):
    return [list(range(first, count, 2)) for first in range(2)]


def exchanged(value):
    link = swapped(value, "cell", 1)
    chip = swapped(value, "cell", 0)
    return link, chip


def per_device(start_block, connectivity, cell_matrices, bounds):
    f32 = jnp.float32
    states, owned = start_block.shape
    shared = owned // 8
    extent = owned + shared
    flag = (lax.axis_index("cell") % 2).astype(jnp.int32).reshape(1)
    weights = scattered(connectivity, cell_matrices, owned, shared)

    peers = lax.axis_size("state")
    line = peers // 2
    bf16 = jnp.bfloat16
    rim = pltpu.VMEM((states, 2 * shared), f32)
    core = pltpu.VMEM((states, owned - shared), f32)
    scratch = [pltpu.VMEM((states, extent), bf16)]
    first = kernel(first_body, 1, (rim, core, rim), scratch)
    edge_step = kernel(edge_body, 2, (rim, rim), [])
    inner_step = kernel(inner_body, 1, (core, rim), scratch)
    lows = pltpu.VMEM((line, states, owned), bf16)
    last_edge = kernel(last_edge_body, 1, (rim, lows, rim), [])
    out = jax.ShapeDtypeStruct((states, owned), f32)
    last_inner = kernel(last_inner_body, 0, (out, core), scratch)

    lowest, cut, upper = (bounds[0], bounds[1], bounds[2])
    half = (upper - cut) / 2.0
    centre = (upper + cut) / 2.0
    sigma = half / (lowest - centre)
    tau = 2.0 / sigma
    coefs = [jnp.stack([sigma / half, -centre * (sigma / half), jnp.zeros((), f32)])]
    for _ in range(2, DEGREE + 1):
        sigma_new = 1.0 / (tau - sigma)
        scale = 2.0 * sigma_new / half
        coefs.append(jnp.stack([scale, -centre * scale, -(sigma * sigma_new)]))
        sigma = sigma_new

    ghost = passed_along(start_block[:, :shared].astype(bf16), "cell", -1)
    edge, inner, fresh = first(coefs[0], start_block, ghost, weights)
    before = ()
    for number, coef in enumerate(coefs):
        link, chip = exchanged(fresh)
        upcoming, ahead = inner_step(coef, edge, inner, weights, *before)
        before, inner = (inner,), upcoming
        if number + 1 < len(coefs):
            edge, fresh = edge_step(
                flag, coefs[number + 1], fresh, link, chip, ahead, edge, weights
            )
    edge, low, edge_product = last_edge(flag, fresh, link, chip, inner, ahead, weights)
    incoming = passed_along(edge_product, "cell", 1)
    lows = lax.all_to_all(low, "state", 0, 0, axis_index_groups=alternate(peers), tiled=True)
    filtered, inner_product = last_inner(edge, inner, weights)
    lows = lows.reshape(line * states, owned)
    shape = pltpu.VMEM((states, owned), bf16)
    image = kernel(finish_body, 0, shape, [])(
        edge_product, inner_product, incoming
    )
    neighbour = swapped(image, "state", 0)

    count = lax.axis_size("cell")
    half = (lax.axis_index("state") % 2).astype(jnp.int32).reshape(1)
    number = line * states // 32
    both = pltpu.VMEM((2, number, 8, 2 * states), f32)
    keep, handed = kernel(project_body, 1, (both, both), [])(flag, lows, image, neighbour)
    part = pltpu.VMEM((number, 8, 2 * states), f32)
    own, other = kernel(add_body, 0, (part, part), [])(keep, swapped(handed, "cell", 0))
    received = swapped(other, "state", 0)
    shape = pltpu.VMEM((number // 2, 2, 2, 8, 2 * states), f32)
    pieces = kernel(place_body, 1, shape, [])(half, own, received)
    pieces = pieces.reshape(2 * number, 8, 2 * states)
    arrived = lax.all_to_all(
        pieces, "cell", 0, 0, axis_index_groups=alternate(count), tiled=True
    )
    rows = peers * states // count
    total = jnp.sum(arrived.reshape(count // 2, rows // 16, 8, 2, states), axis=0)
    projected = jnp.swapaxes(total, 1, 2).reshape(rows, states)
    return (filtered, projected)


def solution(mesh):
    in_specs = (P("state", "cell"), P("cell", None), P("cell", None, None), P())
    out_specs = (P("state", "cell"), P("cell", "state"))
    return jax.shard_map(
        per_device, mesh=mesh, in_specs=in_specs, out_specs=out_specs, check_vma=False
    )
```
